32 devices in a mesh: section: 2 (over core), dp: 8 (over z, x), seq: 2 (over y).
Axes of the slice: x: 2, y: 2, z: 4, core: 2. Of those that a mesh axis runs over, the one named last changes fastest.
Arguments:
- image_in: bfloat16 [2, 8, 128, 1536], P(None, 'dp', 'seq'), may hold values from -6 to 6
- text_in: bfloat16 [2, 8, 64, 1536], P(None, 'dp', 'seq'), may hold values from -6 to 6
- image_cot: bfloat16 [2, 8, 128, 1536], P(None, 'dp', 'seq'), may hold values from -6 to 6
- text_cot: bfloat16 [2, 8, 64, 1536], P(None, 'dp', 'seq'), may hold values from -6 to 6
- cond_table: bfloat16 [16, 1536], replicated, may hold values from -6 to 6
- seq_table: int32 [8, 2], replicated, may hold values from 0 to 15, as said below
- text_count: int32 [2, 8, 2], P(None, 'dp'), may hold values from 1 to 32, as said below
- mod_weight: bfloat16 [2, 2, 1536, 9216], P('section', None, 'dp'), may hold values from -0.15625 to 0.15625
- mod_bias: bfloat16 [2, 2, 9216], P('section', None, 'dp'), may hold values from -3 to 3
- qkv_weight: bfloat16 [2, 2, 1536, 4608], P('section', None, 'dp'), may hold values from -0.15625 to 0.15625
- qkv_bias: bfloat16 [2, 2, 4608], P('section', None, 'dp'), may hold values from -1.1953125 to 1.1953125
- qk_gain: bfloat16 [2, 2, 128], P('section', None, 'dp'), may hold values from 0.5 to 1.5
- out_weight: bfloat16 [2, 2, 1536, 1536], P('section', None, 'dp'), may hold values from -1 to 1
- out_bias: bfloat16 [2, 2, 1536], P('section', None, 'dp'), may hold values from -1.796875 to 1.796875
- up_weight: bfloat16 [2, 2, 1536, 6144], P('section', None, 'dp'), may hold values from -0.15625 to 0.15625
- up_bias: bfloat16 [2, 2, 6144], P('section', None, 'dp'), may hold values from -1.796875 to 1.796875
- down_weight: bfloat16 [2, 2, 6144, 1536], P('section', None, 'dp'), may hold values from -0.078125 to 0.078125
- down_bias: bfloat16 [2, 2, 1536], P('section', None, 'dp'), may hold values from -1.796875 to 1.796875
Outputs:
- image_out: bfloat16 [2, 2, 8, 128, 1536], P('section', None, 'dp', 'seq')
- text_out: bfloat16 [2, 2, 8, 64, 1536], P('section', None, 'dp', 'seq')
- image_grad: float32 [2, 2, 8, 128, 1536], P('section', None, 'dp', 'seq')
- text_grad: float32 [2, 2, 8, 64, 1536], P('section', None, 'dp', 'seq')
- modw_grad: float32 [2, 2, 1536, 9216], P('section', None, 'dp')
- modb_grad: float32 [2, 2, 9216], P('section', None, 'dp')
- qkvw_grad: float32 [2, 2, 1536, 4608], P('section', None, 'dp')
- qkvb_grad: float32 [2, 2, 4608], P('section', None, 'dp')
- gain_grad: float32 [2, 2, 128], P('section', None, 'dp')
- outw_grad: float32 [2, 2, 1536, 1536], P('section', None, 'dp')
- outb_grad: float32 [2, 2, 1536], P('section', None, 'dp')
- upw_grad: float32 [2, 2, 1536, 6144], P('section', None, 'dp')
- upb_grad: float32 [2, 2, 6144], P('section', None, 'dp')
- downw_grad: float32 [2, 2, 6144, 1536], P('section', None, 'dp')
- downb_grad: float32 [2, 2, 1536], P('section', None, 'dp')
The draws below stay inside these ranges and needn't reach their ends.
Inputs may be any that keep to these rules, and one draw needn't show every extreme that they name: `seq_table`: each of the 16 sequence numbers stands exactly once. `text_count`: live text rows held by each device of its sequence; some device holds 32 and some holds 1.
All inputs are finite; a program needn't handle non-finite values.
Results may differ from the reference program's by a relative error of at most 0.04.
Values may be sent and summed in bfloat16 or wider, within the bound.
A program may use at most 576 MiB of HBM per device.

```python
import jax
import jax.numpy as jnp
from jax import lax

D = 1536
HEADS = 24
HD = 64
FF = 6144
TXT_DEV = 32
MB = 2
SECTIONS = 2
SLOTS = 8
SPLIT = 2
SEQS = 16
IMG = 128
TXT = 64


def draw_seq_table(key, part):
    return jax.random.permutation(key, SEQS).astype(jnp.int32).reshape(SLOTS, MB)


def draw_text_count(key, part):
    total_cells = MB * SLOTS * SPLIT
    counts = jax.random.randint(key, (total_cells,), 1, TXT_DEV + 1)
    spot_order = jax.random.permutation(jax.random.fold_in(key, 11), total_cells)
    counts = counts.at[spot_order[0]].set(TXT_DEV)
    counts = counts.at[spot_order[1]].set(1)
    return counts.astype(jnp.int32).reshape(MB, SLOTS, SPLIT)


def steps_of(stream_key, shape, shards, smallest, high):
    def one(dim, shards_of):
        steps = jax.random.uniform(jax.random.fold_in(jax.random.fold_in(stream_key, 6), dim), (shards_of,), jnp.float32, smallest / len(shards), high / len(shards))
        return jnp.repeat(jnp.exp(steps), shape[dim] // shards_of).reshape((-1,) + (1,) * (len(shape) - dim - 1))

    factor_of = one(*shards[0])
    for cut in shards[1:]:
        factor_of = factor_of * one(*cut)
    return factor_of


def gaussian(rng, shape, spread, bound, shards=(), kind=jnp.bfloat16):
    result = spread * jax.random.normal(rng, shape, jnp.float32)
    if shards:
        result = result * steps_of(rng, shape, shards, -0.22, 0.18)
    return jnp.clip(result, -bound, bound).astype(kind)


def setup_inputs(seed: int = 0) -> dict:
    splits = jax.random.split(jax.random.key(seed), 19)
    return {
        "image_in": gaussian(splits[0], (MB, SLOTS, IMG, D), 1.0, 6.0, ((1, 8), (2, 2))),
        "text_in": gaussian(splits[1], (MB, SLOTS, TXT, D), 1.0, 6.0, ((1, 8), (2, 2))),
        "image_cot": gaussian(splits[2], (MB, SLOTS, IMG, D), 1.0, 6.0, ((1, 8), (2, 2))),
        "text_cot": gaussian(splits[3], (MB, SLOTS, TXT, D), 1.0, 6.0, ((1, 8), (2, 2))),
        "cond_table": gaussian(splits[4], (SEQS, D), 1.0, 6.0),
        "seq_table": draw_seq_table(jax.random.fold_in(splits[18], 71), 0),
        "text_count": draw_text_count(jax.random.fold_in(splits[18], 71), 0),
        "mod_weight": gaussian(splits[7], (SECTIONS, 2, D, 6 * D), D ** -0.5, 0.15625, ((0, 2), (2, 8))),
        "mod_bias": gaussian(splits[8], (SECTIONS, 2, 6 * D), 0.5, 3.0, ((0, 2), (2, 8))),
        "qkv_weight": gaussian(splits[9], (SECTIONS, 2, D, 3 * D), D ** -0.5, 0.15625, ((0, 2), (2, 8))),
        "qkv_bias": gaussian(splits[10], (SECTIONS, 2, 3 * D), 0.2, 1.1953125, ((0, 2), (2, 8))),
        "qk_gain": jnp.clip(1.0 + 0.1 * jax.random.normal(splits[11], (SECTIONS, 2, 2 * HD), jnp.float32), 0.5, 1.5).astype(jnp.bfloat16),
        "out_weight": gaussian(splits[12], (SECTIONS, 2, D, D), (D // 48) ** -0.5, 1.0, ((0, 2), (2, 8))),
        "out_bias": gaussian(splits[13], (SECTIONS, 2, D), 0.3, 1.796875, ((0, 2), (2, 8))),
        "up_weight": gaussian(splits[14], (SECTIONS, 2, D, FF), D ** -0.5, 0.15625, ((0, 2), (2, 8))),
        "up_bias": gaussian(splits[15], (SECTIONS, 2, FF), 0.3, 1.796875, ((0, 2), (2, 8))),
        "down_weight": gaussian(splits[16], (SECTIONS, 2, FF, D), FF ** -0.5, 0.078125, ((0, 2), (2, 8))),
        "down_bias": gaussian(splits[17], (SECTIONS, 2, D), 0.3, 1.796875, ((0, 2), (2, 8))),
    }


@jax.custom_vjp
def low(v):
    return lax.optimization_barrier(v.astype(jnp.bfloat16)).astype(jnp.float32)

@jax.custom_vjp
def low_back(v):
    return v

def low_keep(v):
    return (low(v), None)

def low_pass(kept, grad):
    return (grad,)

def back_keep(v):
    return (v, None)

def back_low(kept, grad):
    return (low(grad),)
low.defvjp(low_keep, low_pass)
low_back.defvjp(back_keep, back_low)
eps_norm = 1e-06
gelu_coef = 0.7978845608028654
highest = lax.Precision.HIGHEST

def layer_norm(values):
    center = values - lax.optimization_barrier(jnp.mean(values, axis=-1, keepdims=True))
    return center * lax.rsqrt(lax.optimization_barrier(jnp.mean(center * center, axis=-1, keepdims=True)) + eps_norm)

def head_norm(values, gain_vec):
    return values * lax.rsqrt(lax.optimization_barrier(jnp.mean(values * values, axis=-1, keepdims=True)) + eps_norm) * gain_vec

def gelu_tanh(values):
    return 0.5 * values * (1.0 + jnp.tanh(gelu_coef * (values + 0.044715 * values * values * values)))

def joint_layer(image_x, text_x, live_mask, cond_vec, params):
    mod_w, mod_b, qkv_w, qkv_b, gains, out_w, out_b, up_w, up_b, down_w, down_b = params
    inputs = (image_x, text_x)
    mod_list = []
    query_list = []
    key_list = []
    value_list = []
    for stream in range(2):
        mod_rows = (jnp.dot(cond_vec, mod_w[stream], precision=highest) + mod_b[stream]).reshape(6, D)
        mod_list.append(mod_rows)
        hidden = low(layer_norm(inputs[stream]) * (1.0 + mod_rows[1]) + mod_rows[0])
        packed = low_back(low(jnp.dot(hidden, qkv_w[stream], precision=highest) + qkv_b[stream]))
        packed = packed.reshape(-1, HEADS, 3, HD)
        query_list.append(low(head_norm(packed[:, :, 0], gains[stream, :HD])))
        key_list.append(low(head_norm(packed[:, :, 1], gains[stream, HD:])))
        value_list.append(packed[:, :, 2])
    query_rows = jnp.concatenate(query_list, axis=0)
    key_rows = jnp.concatenate(key_list, axis=0)
    value_rows = jnp.concatenate(value_list, axis=0)
    key_live = jnp.concatenate([jnp.ones((IMG,), jnp.float32), live_mask])
    scores = low_back(jnp.einsum('qhd,khd->hqk', query_rows, key_rows, precision=highest) * 0.125)
    exp_scores = jnp.exp(scores) * key_live
    probs_low = low(exp_scores / lax.optimization_barrier(jnp.sum(exp_scores, axis=-1, keepdims=True)))
    attended = low_back(low(jnp.einsum('hqk,khd->qhd', probs_low, value_rows, precision=highest)))
    attended = attended.reshape(-1, D)
    results = []
    for stream in range(2):
        mod_rows = mod_list[stream]
        if stream == 0:
            rows_here = attended[:IMG]
        else:
            rows_here = attended[IMG:]
        branch = low_back(jnp.dot(rows_here, out_w[stream], precision=highest) + out_b[stream])
        middle = inputs[stream] + mod_rows[2] * branch
        hidden_mid = low(layer_norm(middle) * (1.0 + mod_rows[4]) + mod_rows[3])
        pre_act = low_back(jnp.dot(hidden_mid, up_w[stream], precision=highest) + up_b[stream])
        active = low(gelu_tanh(pre_act))
        mlp_out = low_back(jnp.dot(active, down_w[stream], precision=highest) + down_b[stream])
        results.append(middle + mod_rows[5] * mlp_out)
    return (results[0], results[1] * live_mask[:, None])

def reference(image_in, text_in, image_cot, text_cot, cond_table, seq_table, text_count, mod_weight, mod_bias, qkv_weight, qkv_bias, qk_gain, out_weight, out_bias, up_weight, up_bias, down_weight, down_bias):
    total_seqs = MB * SLOTS
    group_size = 1
    for size_try in (8, 4, 2):
        if group_size == 1 and total_seqs % size_try == 0:
            group_size = size_try
    blocks = total_seqs // group_size
    seq_ids = seq_table.T.reshape(-1).astype(jnp.int32)
    cond_vecs = low(jax.nn.silu(cond_table.astype(jnp.float32)[seq_ids]))
    positions = jnp.arange(TXT)
    counts = text_count.reshape(total_seqs, SPLIT)
    live_mask = ((positions % TXT_DEV)[None, :] < counts[:, positions // TXT_DEV]).astype(jnp.float32)
    params = tuple((array.astype(jnp.float32) for array in (mod_weight, mod_bias, qkv_weight, qkv_bias, qk_gain, out_weight, out_bias, up_weight, up_bias, down_weight, down_bias)))

    def group_fn(layer_params, batch_part):
        return jax.vmap(joint_layer, in_axes=(0, 0, 0, 0, None))(batch_part[0], batch_part[1], batch_part[2], batch_part[3], layer_params)
    saved_fn = jax.checkpoint(group_fn)

    def run_layer(image_x, text_x, layer_params):
        shaped = (image_x.reshape(blocks, group_size, IMG, D), text_x.reshape(blocks, group_size, TXT, D), live_mask.reshape(blocks, group_size, TXT), cond_vecs.reshape(blocks, group_size, D))
        image_y, text_y = lax.map(lambda batch_part: saved_fn(layer_params, batch_part), shaped)
        return (image_y.reshape(total_seqs, IMG, D), text_y.reshape(total_seqs, TXT, D))

    def forward(image_x, text_x, image_zero, text_zero, *weights):
        first_layer = tuple((array[0] for array in weights))
        second = tuple((array[1] for array in weights))
        image_one, text_one = run_layer(image_x, text_x, first_layer)
        image_one = low_back(low(image_one) + image_zero)
        text_one = low_back(low(text_one) + text_zero)
        image_two, text_two = run_layer(image_one, text_one, second)
        return ((image_two, text_two), (image_one, text_one))
    image_x = image_in.astype(jnp.float32).reshape(total_seqs, IMG, D)
    text_x = text_in.astype(jnp.float32).reshape(total_seqs, TXT, D)
    zero_image = jnp.zeros((total_seqs, IMG, D), jnp.float32)
    zero_text = jnp.zeros((total_seqs, TXT, D), jnp.float32)
    outputs, pullback, kept_mid = jax.vjp(forward, image_x, text_x, zero_image, zero_text, *params, has_aux=True)
    cot_pair = (image_cot.astype(jnp.float32).reshape(total_seqs, IMG, D), text_cot.astype(jnp.float32).reshape(total_seqs, TXT, D))
    gradients = pullback(cot_pair)
    image_shape = (SECTIONS, MB, SLOTS, IMG, D)
    text_shape = (SECTIONS, MB, SLOTS, TXT, D)
    image_out = jnp.stack([kept_mid[0], outputs[0]]).reshape(image_shape).astype(jnp.bfloat16)
    text_out = jnp.stack([kept_mid[1], outputs[1]]).reshape(text_shape).astype(jnp.bfloat16)
    image_grad = jnp.stack([gradients[0], gradients[2]]).reshape(image_shape)
    text_grad = jnp.stack([gradients[1], gradients[3]]).reshape(text_shape)
    return (image_out, text_out, image_grad, text_grad, gradients[4], gradients[5], gradients[6], gradients[7], gradients[8], gradients[9], gradients[10], gradients[11], gradients[12], gradients[13], gradients[14])
```

```python
import functools

import jax
import jax.numpy as jnp
from jax import lax
from jax.experimental import pallas as pl
from jax.experimental.pallas import tpu as pltpu
from jax.sharding import PartitionSpec as P

HEADS = 24
HD = 64
TP = 8


eps_norm = 1e-06
gelu_coef = 0.7978845608028654
MESH = pl.DeviceIdType.MESH


def layer_norm(values):
    center = values - jnp.mean(values, axis=-1, keepdims=True)
    inv_std = lax.rsqrt(jnp.mean(center * center, axis=-1, keepdims=True) + eps_norm)
    return (center * inv_std, inv_std)


def norm_back(gradient, normed, inv_std):
    return inv_std * (
        gradient
        - jnp.mean(gradient, axis=-1, keepdims=True)
        - normed * jnp.mean(gradient * normed, axis=-1, keepdims=True)
    )


def head_norm(raw_vals):
    inv_std = lax.rsqrt(jnp.mean(raw_vals * raw_vals, axis=-1, keepdims=True) + eps_norm)
    return (raw_vals * inv_std, inv_std)


def head_back(gradient, unit_vals, inv_std):
    return inv_std * (gradient - unit_vals * jnp.mean(gradient * unit_vals, axis=-1, keepdims=True))


def gelu_both(pre_act):
    inner_arg = gelu_coef * (pre_act + 0.044715 * pre_act * pre_act * pre_act)
    tanh_val = jnp.tanh(inner_arg)
    act_value = 0.5 * pre_act * (1.0 + tanh_val)
    act_slope = 0.5 * (1.0 + tanh_val) + 0.5 * pre_act * (1.0 - tanh_val * tanh_val) * gelu_coef * (
        1.0 + 3.0 * 0.044715 * pre_act * pre_act
    )
    return (act_value, act_slope)


def mat(left, right):
    return lax.dot_general(
        left, right, (((1,), (0,)), ((), ())), preferred_element_type=jnp.float32
    )


def rows_product(left_rows, right_rows):
    return lax.dot_general(
        left_rows, right_rows, (((0,), (0,)), ((), ())), preferred_element_type=jnp.float32
    )


def back_product(grad_rows, weight_mat):
    return lax.dot_general(
        grad_rows, weight_mat, (((1,), (1,)), ((), ())), preferred_element_type=jnp.float32
    )


def ring_place(tp):
    row, col = (tp // 2, tp % 2)
    return row + col * (TP - 1 - 2 * row)


def ring_member(place):
    far = place // (TP // 2)
    row = place + far * (TP - 1 - 2 * place)
    return 2 * row + far


def ring_of(groups):
    dp_index = lax.axis_index("dp")
    sense = 1 - 2 * lax.axis_index("section")
    place = ring_place(dp_index // groups)
    group = dp_index % groups

    def member(steps):
        return ring_member((place + 2 * TP + sense * steps) % TP)

    sides = (member(1) * groups + group, member(-1) * groups + group)
    return (member, sides)


def greet(sides):
    barrier = pltpu.get_barrier_semaphore()
    for side in sides:
        pl.semaphore_signal(barrier, inc=1, device_id={"dp": side}, device_id_type=MESH)
    pl.semaphore_wait(barrier, 2)


def gather_kernel(groups, img_ref, txt_ref, img_out, txt_out, send_sem, recv_sem):
    member, sides = ring_of(groups)
    half = img_ref.shape[0] // 2
    pieces = ((img_ref, img_out, 0), (img_ref, img_out, half), (txt_ref, txt_out, 0))

    def copy_of(side, hop, piece):
        source_ref, target_ref, start = pieces[piece]
        origin = member(-hop if side == 0 else hop)
        rows = pl.ds(start, half)
        source = source_ref.at[rows] if hop == 0 else target_ref.at[origin, rows]
        return pltpu.make_async_remote_copy(
            src_ref=source,
            dst_ref=target_ref.at[origin, rows],
            send_sem=send_sem.at[side, hop, piece],
            recv_sem=recv_sem.at[side, hop, piece],
            device_id={"dp": sides[side]},
            device_id_type=MESH,
        )

    def moves(side, hop, piece):
        return hop < 3 or (piece < 2) == (side == 0)

    greet(sides)
    for hop in range(4):
        for piece in range(3):
            for side in range(2):
                if moves(side, hop, piece):
                    if hop > 0:
                        copy_of(side, hop - 1, piece).wait_recv()
                    copy_of(side, hop, piece).start()
        if hop == 0:
            me = member(0)
            img_out[me] = img_ref[...]
            txt_out[me] = txt_ref[...]
    for piece in range(3):
        for side in range(2):
            copy_of(side, 3 if moves(side, 3, piece) else 2, piece).wait_recv()
    for hop in range(4):
        for piece in range(3):
            for side in range(2):
                if moves(side, hop, piece):
                    copy_of(side, hop, piece).wait_send()


def gather_rows(img_rows, txt_rows, groups):
    return pl.pallas_call(
        functools.partial(gather_kernel, groups),
        out_shape=(
            jax.ShapeDtypeStruct((TP,) + img_rows.shape, img_rows.dtype),
            jax.ShapeDtypeStruct((TP,) + txt_rows.shape, txt_rows.dtype),
        ),
        in_specs=[pl.BlockSpec(memory_space=pltpu.VMEM)] * 2,
        out_specs=(pl.BlockSpec(memory_space=pltpu.VMEM),) * 2,
        scratch_shapes=[pltpu.SemaphoreType.DMA((2, 4, 3)), pltpu.SemaphoreType.DMA((2, 4, 3))],
        compiler_params=pltpu.CompilerParams(collective_id=1, has_side_effects=True),
    )(img_rows, txt_rows)


def scatter_kernel(groups, piece_rows, *refs):
    count = len(piece_rows)
    part_refs = refs[:count]
    out_ref, recv, send, send_sem, recv_sem = refs[count:]
    member, sides = ring_of(groups)
    pieces = []
    row = 0
    for index, sizes in enumerate(piece_rows):
        start = 0
        for size in sizes:
            pieces.append((part_refs[index], start, row, size))
            start += size
            row += size

    def moves(side, hop, piece):
        return hop > 0 or (piece < 2) == (side == 0)

    def dest_of(side, hop):
        return member(4 - hop if side == 0 else hop - 4)

    def copy_of(side, hop, piece):
        part_ref, start, row, size = pieces[piece]
        if hop == 0:
            source = part_ref.at[dest_of(side, hop), pl.ds(start, size)]
        elif moves(side, hop - 1, piece):
            source = send.at[side, hop, pl.ds(row, size)]
        else:
            source = part_ref.at[dest_of(side, hop), pl.ds(start, size)]
        return pltpu.make_async_remote_copy(
            src_ref=source,
            dst_ref=recv.at[side, hop, pl.ds(row, size)],
            send_sem=send_sem.at[side, hop, piece],
            recv_sem=recv_sem.at[side, hop, piece],
            device_id={"dp": sides[side]},
            device_id_type=MESH,
        )

    greet(sides)
    for hop in range(4):
        for piece in range(len(pieces)):
            for side in range(2):
                if moves(side, hop, piece):
                    if hop > 0 and moves(side, hop - 1, piece):
                        part_ref, start, row, size = pieces[piece]
                        copy_of(side, hop - 1, piece).wait_recv()
                        send[side, hop, pl.ds(row, size)] = (
                            recv[side, hop - 1, pl.ds(row, size)].astype(jnp.float32)
                            + part_ref[dest_of(side, hop), pl.ds(start, size)].astype(jnp.float32)
                        ).astype(send.dtype)
                    copy_of(side, hop, piece).start()
    me = member(0)
    for piece in range(len(pieces)):
        part_ref, start, row, size = pieces[piece]
        total = part_ref[me, pl.ds(start, size)].astype(jnp.float32)
        for side in range(2):
            copy_of(side, 3, piece).wait_recv()
            total = total + recv[side, 3, pl.ds(row, size)].astype(jnp.float32)
        out_ref[pl.ds(row, size)] = total
    for hop in range(4):
        for piece in range(len(pieces)):
            for side in range(2):
                if moves(side, hop, piece):
                    copy_of(side, hop, piece).wait_send()


def scatter_sums(parts, piece_rows, groups, collective):
    rows = sum(sum(sizes) for sizes in piece_rows)
    count = sum(len(sizes) for sizes in piece_rows)
    width = parts[0].shape[-1]
    return pl.pallas_call(
        functools.partial(scatter_kernel, groups, piece_rows),
        out_shape=jax.ShapeDtypeStruct((rows, width), jnp.float32),
        in_specs=[pl.BlockSpec(memory_space=pltpu.VMEM)] * len(parts),
        out_specs=pl.BlockSpec(memory_space=pltpu.VMEM),
        scratch_shapes=[
            pltpu.VMEM((2, 4, rows, width), jnp.bfloat16),
            pltpu.VMEM((2, 4, rows, width), jnp.bfloat16),
            pltpu.SemaphoreType.DMA((2, 4, count)),
            pltpu.SemaphoreType.DMA((2, 4, count)),
        ],
        compiler_params=pltpu.CompilerParams(collective_id=collective, has_side_effects=True),
    )(*parts)


def body(
    image_in,
    text_in,
    image_cot,
    text_cot,
    cond_table,
    seq_table,
    text_count,
    mod_weight,
    mod_bias,
    qkv_weight,
    qkv_bias,
    qk_gain,
    out_weight,
    out_bias,
    up_weight,
    up_bias,
    down_weight,
    down_bias,
):
    core = lax.axis_index("section")
    dp_index = lax.axis_index("dp")
    seq_index = lax.axis_index("seq")
    data_parts = lax.axis_size("dp")
    groups = data_parts // TP
    tp_index = dp_index // groups
    group_index = dp_index % groups
    layers = lax.axis_size("section")
    first = core == 0
    batches = image_in.shape[0]
    image_rows = image_in.shape[2]
    text_rows = text_in.shape[2]
    width = image_in.shape[3]
    local_heads = HEADS // TP
    seq_keys = 2 * (image_rows + text_rows)
    key_share = width // TP
    tp_groups = [[t * groups + g for t in range(TP)] for g in range(groups)]
    row_groups = [[t * groups + g for g in range(groups)] for t in range(TP)]
    swap = [(0, 1), (1, 0)]

    def whole_share(value, axis):
        if groups == 1:
            return value
        return lax.all_gather(value, "dp", axis=axis, tiled=True, axis_index_groups=row_groups)

    def across_tp(value, split_axis, concat_axis):
        return lax.all_to_all(
            value, "dp", split_axis, concat_axis, axis_index_groups=tp_groups, tiled=True
        )

    def both_layers(own):
        other = lax.ppermute(own, "section", swap)
        return (jnp.where(first, own, other), jnp.where(first, other, own))

    trade = []
    for d in range(data_parts):
        for s in range(2):
            t, g = (d // groups, d % groups)
            held = (t - t % 2 + s) * groups + g
            trade.append((held * 2 + t % 2, d * 2 + s))

    def to_work(image, text):
        rows = jnp.concatenate(
            [
                lax.dynamic_index_in_dim(image, core, 0, keepdims=False)[0],
                lax.dynamic_index_in_dim(text, core, 0, keepdims=False)[0],
            ],
            axis=0,
        )
        return lax.ppermute(rows, ("dp", "seq"), trade)

    start_rows = to_work(image_in, text_in)

    mod_mats = whole_share(mod_weight[0], 1)
    all_tp = jnp.arange(TP)
    held_tp = all_tp - all_tp % 2 + seq_index
    held_ids = jnp.take(seq_table, held_tp * groups + group_index, axis=0).reshape(-1)
    held_cond = jax.nn.silu(jnp.take(cond_table, held_ids, axis=0).astype(jnp.float32)).astype(
        jnp.bfloat16
    )
    cond_cols = lax.dynamic_slice_in_dim(held_cond, tp_index * key_share, key_share, 1)
    partial_mod = jnp.einsum("rd,sdk->rsk", cond_cols, mod_mats, preferred_element_type=jnp.float32)
    mod_add = whole_share(mod_bias[0], 1).astype(jnp.float32)
    mod_span = mod_add.shape[1]
    mod_cols = partial_mod.shape[2]
    mod_place = lax.dynamic_update_slice(
        jnp.zeros((2, mod_cols), jnp.float32), mod_add, (0, tp_index * mod_span)
    )
    mod_rows_each = batches * 2 * 6
    partial_mod = (partial_mod + mod_place[None]).astype(jnp.bfloat16)
    partial_mod = partial_mod.reshape(TP, mod_rows_each, width)
    own_gain = whole_share(qk_gain[0], 1)
    gain_span = own_gain.shape[1]
    gain_place = lax.dynamic_update_slice(
        jnp.zeros((2, TP * gain_span), jnp.bfloat16), own_gain, (0, tp_index * gain_span)
    ).reshape(-1)
    count_place = lax.dynamic_update_slice(
        jnp.zeros((TP, batches, 2), jnp.bfloat16),
        text_count.transpose(1, 0, 2).astype(jnp.bfloat16),
        (tp_index, 0, 0),
    ).reshape(-1)
    extra = jnp.concatenate([gain_place, count_place])
    extra = jnp.zeros((8, width), jnp.bfloat16).at[0, : extra.shape[0]].set(extra)
    partial_mod = jnp.concatenate(
        [partial_mod, jnp.broadcast_to(extra[None], (TP, 8, width))], axis=1
    )
    mod_sums = scatter_sums((partial_mod,), ((16, 16, 0)[:2],), groups, 3)
    gain_size = 2 * TP * gain_span
    counts = mod_sums[mod_rows_each, gain_size : gain_size + TP * batches * 2].reshape(
        TP, batches, 2
    )
    layer_mods = mod_sums[:mod_rows_each].reshape(batches, 12, width)
    own_pack = jnp.concatenate(
        [
            lax.dynamic_index_in_dim(layer_mods, core, 0, keepdims=False),
            mod_sums[mod_rows_each : mod_rows_each + 1],
        ]
    )
    sent_pack = jnp.concatenate(
        [
            lax.dynamic_index_in_dim(layer_mods, 1 - core, 0, keepdims=False),
            mod_sums[mod_rows_each : mod_rows_each + 1],
        ]
    )
    other_pack = lax.ppermute(sent_pack, "section", swap)
    packs = (
        jnp.where(first, own_pack, other_pack),
        jnp.where(first, other_pack, own_pack),
    )
    mods = tuple(pack[:12].reshape(2, 6, width) for pack in packs)
    gains = tuple(pack[12, :gain_size].reshape(2, 2 * HD) for pack in packs)

    my_counts = lax.dynamic_index_in_dim(counts, core, 1, keepdims=False)
    group_counts = jnp.take_along_axis(
        jnp.take(my_counts, held_tp, axis=0), (all_tp % 2)[:, None], axis=1
    )[:, 0]
    text_pos = jnp.arange(text_rows).astype(jnp.float32)
    text_live = (text_pos[None, :] < group_counts[:, None]).astype(jnp.float32)
    key_mask = jnp.concatenate(
        [jnp.ones((TP, image_rows), jnp.float32), text_live], axis=1
    ).reshape(TP // 2, seq_keys)
    own_live = jnp.concatenate(
        [
            jnp.ones((image_rows,), jnp.float32),
            lax.dynamic_index_in_dim(text_live, tp_index, 0, keepdims=False),
        ]
    )[:, None]

    qkv_mats = both_layers(across_tp(whole_share(qkv_weight[0], 1), 2, 1))
    out_mats = both_layers(whole_share(out_weight[0], 1))
    up_mats = both_layers(across_tp(whole_share(up_weight[0], 1), 2, 1))
    down_mats = both_layers(whole_share(down_weight[0], 1))
    own_adds = [
        whole_share(value[0], 1).astype(jnp.float32)
        for value in (qkv_bias, out_bias, up_bias, down_bias)
    ]
    add_sizes = [value.shape[1] for value in own_adds]
    adds = both_layers(jnp.concatenate(own_adds, axis=1))

    def split_adds(layer):
        parts = []
        start = 0
        for size in add_sizes:
            parts.append(adds[layer][:, start : start + size])
            start += size
        return parts

    def placed(value):
        return lax.dynamic_update_slice(
            jnp.zeros((width,), jnp.float32), value, (tp_index * value.shape[0],)
        )

    def gathered(rows):
        img, txt = gather_rows(rows[:image_rows], rows[image_rows:], groups)
        return (img.reshape(-1, width), txt.reshape(-1, width))

    def scattered(parts):
        half = image_rows // 2
        return scatter_sums(
            (
                parts[0].astype(jnp.bfloat16).reshape(TP, image_rows, width),
                parts[1].astype(jnp.bfloat16).reshape(TP, text_rows, width),
            ),
            ((half, half), (text_rows,)),
            groups,
            2,
        )

    def by_stream(mod_rows, index):
        return jnp.concatenate(
            [
                jnp.broadcast_to(mod_rows[0, index], (image_rows, width)),
                jnp.broadcast_to(mod_rows[1, index], (text_rows, width)),
            ]
        )

    def joined(parts, columns):
        return jnp.concatenate(
            [
                parts[0].reshape(TP, image_rows, columns),
                parts[1].reshape(TP, text_rows, columns),
            ],
            axis=1,
        )

    def parted(value):
        columns = value.shape[-1]
        value = value.reshape(TP, image_rows + text_rows, columns)
        return (
            value[:, :image_rows].reshape(-1, columns),
            value[:, image_rows:].reshape(-1, columns),
        )

    def spread_gain(gain_rows, offset):
        half = jnp.concatenate(
            [
                jnp.broadcast_to(gain_rows[0, offset : offset + HD], (image_rows, HD)),
                jnp.broadcast_to(gain_rows[1, offset : offset + HD], (text_rows, HD)),
            ]
        )
        return jnp.concatenate([half, half])[None, :, None, :]

    def head_inputs(heads, gain_rows):
        query_unit, query_inv = head_norm(heads[:, :, :, 0].astype(jnp.float32))
        key_unit, key_inv = head_norm(heads[:, :, :, 1].astype(jnp.float32))
        query_low = (query_unit * spread_gain(gain_rows, 0)).astype(jnp.bfloat16)
        key_low = (key_unit * spread_gain(gain_rows, HD)).astype(jnp.bfloat16)
        return (query_unit, query_inv, key_unit, key_inv, query_low, key_low)

    def forward(layer, rows):
        mod_rows = mods[layer]
        qkv_add, out_add, up_add, down_add = split_adds(layer)
        values = rows.astype(jnp.float32)
        normed, inv_std = layer_norm(values)
        hidden = (normed * (1.0 + by_stream(mod_rows, 1)) + by_stream(mod_rows, 0)).astype(
            jnp.bfloat16
        )
        hidden_all = gathered(hidden)
        packed = [
            (mat(hidden_all[t], qkv_mats[layer][t]) + qkv_add[t]).astype(jnp.bfloat16)
            for t in range(2)
        ]
        heads = joined(packed, packed[0].shape[-1]).reshape(
            TP // 2, seq_keys, local_heads, 3, HD
        )
        _, _, _, _, query_low, key_low = head_inputs(heads, gains[layer])
        scores = (
            jnp.einsum(
                "bqhd,bkhd->bhqk", query_low, key_low, preferred_element_type=jnp.float32
            )
            * 0.125
        )
        exp_scores = jnp.exp(scores) * key_mask[:, None, None, :]
        denom_sum = jnp.sum(exp_scores, axis=-1, keepdims=True)
        probs_low = (exp_scores / denom_sum).astype(jnp.bfloat16)
        attended = jnp.einsum(
            "bhqk,bkhd->bqhd", probs_low, heads[:, :, :, 2], preferred_element_type=jnp.float32
        ).astype(jnp.bfloat16)
        attended = parted(attended.reshape(TP // 2, seq_keys, local_heads * HD))
        branch = scattered(
            [mat(attended[t], out_mats[layer][t]) + placed(out_add[t]) for t in range(2)]
        )
        middle = values + by_stream(mod_rows, 2) * branch
        normed_mid, inv_mid = layer_norm(middle)
        hidden_mid = (
            normed_mid * (1.0 + by_stream(mod_rows, 4)) + by_stream(mod_rows, 3)
        ).astype(jnp.bfloat16)
        mid_all = gathered(hidden_mid)
        acts = []
        slopes = []
        for t in range(2):
            act_value, act_slope = gelu_both(mat(mid_all[t], up_mats[layer][t]) + up_add[t])
            acts.append(act_value.astype(jnp.bfloat16))
            slopes.append(act_slope)
        mlp_out = scattered(
            [mat(acts[t], down_mats[layer][t]) + placed(down_add[t]) for t in range(2)]
        )
        result = (middle + by_stream(mod_rows, 5) * mlp_out) * own_live
        saved = (
            normed,
            inv_std,
            hidden_all,
            heads,
            denom_sum,
            attended,
            branch,
            normed_mid,
            inv_mid,
            mid_all,
            acts,
            slopes,
            mlp_out,
        )
        return (result.astype(jnp.bfloat16), saved)

    def stream_sums(value):
        return jnp.stack(
            [jnp.sum(value[:image_rows], axis=0), jnp.sum(value[image_rows:], axis=0)]
        )

    def backward(layer, grad_rows, saved):
        (
            normed,
            inv_std,
            hidden_all,
            heads,
            denom_sum,
            attended,
            branch,
            normed_mid,
            inv_mid,
            mid_all,
            acts,
            slopes,
            mlp_out,
        ) = saved
        mod_rows = mods[layer]
        grad_out = grad_rows * own_live
        gate_two = stream_sums(grad_out * mlp_out)
        mlp_all = gathered((by_stream(mod_rows, 5) * grad_out).astype(jnp.bfloat16))
        pre_grads = [
            (back_product(mlp_all[t], down_mats[layer][t]) * slopes[t]).astype(jnp.bfloat16)
            for t in range(2)
        ]
        hidden_grad = scattered([back_product(pre_grads[t], up_mats[layer][t]) for t in range(2)])
        down_grads = [rows_product(acts[t], mlp_all[t]).astype(jnp.bfloat16) for t in range(2)]
        up_grads = [rows_product(mid_all[t], pre_grads[t]).astype(jnp.bfloat16) for t in range(2)]
        scale_two = stream_sums(hidden_grad * normed_mid)
        shift_two = stream_sums(hidden_grad)
        middle_grad = grad_out + norm_back(
            hidden_grad * (1.0 + by_stream(mod_rows, 4)), normed_mid, inv_mid
        )
        gate_one = stream_sums(middle_grad * branch)
        branch_all = gathered((by_stream(mod_rows, 2) * middle_grad).astype(jnp.bfloat16))
        attn_grads = [
            back_product(branch_all[t], out_mats[layer][t]).astype(jnp.bfloat16) for t in range(2)
        ]
        out_grads = [rows_product(attended[t], branch_all[t]).astype(jnp.bfloat16) for t in range(2)]
        out_grad = joined(attn_grads, local_heads * HD).reshape(
            TP // 2, seq_keys, local_heads, HD
        )
        query_unit, query_inv, key_unit, key_inv, query_low, key_low = head_inputs(
            heads, gains[layer]
        )
        scores = (
            jnp.einsum(
                "bqhd,bkhd->bhqk", query_low, key_low, preferred_element_type=jnp.float32
            )
            * 0.125
        )
        probs = jnp.exp(scores) * key_mask[:, None, None, :] / denom_sum
        prob_grad = jnp.einsum(
            "bqhd,bkhd->bhqk", out_grad, heads[:, :, :, 2], preferred_element_type=jnp.float32
        )
        row_dot = jnp.sum(probs * prob_grad, axis=-1, keepdims=True)
        score_grad = (probs * (prob_grad - row_dot)).astype(jnp.bfloat16)
        value_grad = jnp.einsum(
            "bhqk,bqhd->bkhd",
            probs.astype(jnp.bfloat16),
            out_grad,
            preferred_element_type=jnp.float32,
        )
        query_grad = (
            jnp.einsum("bhqk,bkhd->bqhd", score_grad, key_low, preferred_element_type=jnp.float32)
            * 0.125
        )
        key_grad = (
            jnp.einsum("bhqk,bqhd->bkhd", score_grad, query_low, preferred_element_type=jnp.float32)
            * 0.125
        )

        def gain_sums(grad, unit):
            row_sums = jnp.sum(grad * unit, axis=(0, 2)).reshape(2, image_rows + text_rows, HD)
            return jnp.stack(
                [
                    jnp.sum(row_sums[:, :image_rows], axis=(0, 1)),
                    jnp.sum(row_sums[:, image_rows:], axis=(0, 1)),
                ]
            )

        gain_grad = jnp.concatenate(
            [gain_sums(query_grad, query_unit), gain_sums(key_grad, key_unit)], axis=1
        )
        packed_grad = jnp.stack(
            [
                head_back(query_grad * spread_gain(gains[layer], 0), query_unit, query_inv),
                head_back(key_grad * spread_gain(gains[layer], HD), key_unit, key_inv),
                value_grad,
            ],
            axis=3,
        ).astype(jnp.bfloat16)
        qkv_grads = parted(packed_grad.reshape(TP // 2, seq_keys, local_heads * 3 * HD))
        hidden_grad = scattered([back_product(qkv_grads[t], qkv_mats[layer][t]) for t in range(2)])
        weight_grads = [
            rows_product(hidden_all[t], qkv_grads[t]).astype(jnp.bfloat16) for t in range(2)
        ]
        scale_one = stream_sums(hidden_grad * normed)
        shift_one = stream_sums(hidden_grad)
        grad_in = middle_grad + norm_back(
            hidden_grad * (1.0 + by_stream(mod_rows, 1)), normed, inv_std
        )
        mod_grad = jnp.stack(
            [shift_one, scale_one, gate_one, shift_two, scale_two, gate_two], axis=1
        )

        def own_columns(value):
            share = value.shape[1] // TP
            return lax.dynamic_slice_in_dim(value, tp_index * share, share, 1)

        def row_sums(values):
            return jnp.stack([jnp.sum(value.astype(jnp.float32), axis=0) for value in values])

        bias_grads = (
            row_sums(qkv_grads),
            own_columns(row_sums(branch_all)),
            row_sums(pre_grads),
            own_columns(row_sums(mlp_all)),
        )
        return (
            grad_in,
            mod_grad,
            gain_grad,
            bias_grads,
            (
                jnp.stack(weight_grads),
                jnp.stack(out_grads),
                jnp.stack(up_grads),
                jnp.stack(down_grads),
            ),
        )

    def settle(value, by_columns):
        columns = value.shape[-1]
        blocks = TP if by_columns else 1
        value = value.reshape(2, blocks, -1, columns)
        if groups > 1:
            value = lax.psum_scatter(
                value, "dp", scatter_dimension=2, axis_index_groups=row_groups, tiled=True
            )
        half = value.shape[2] // 2
        sent = lax.dynamic_slice_in_dim(value, (1 - core) * half, half, 2)
        kept = lax.dynamic_slice_in_dim(value, core * half, half, 2)
        kept = (
            kept.astype(jnp.float32) + lax.ppermute(sent, "section", swap).astype(jnp.float32)
        ).astype(jnp.bfloat16)
        sent = lax.dynamic_index_in_dim(kept, 1 - seq_index, 0, keepdims=False)
        kept = lax.dynamic_index_in_dim(kept, seq_index, 0, keepdims=False)
        kept = (
            kept.astype(jnp.float32) + lax.ppermute(sent, "seq", swap).astype(jnp.float32)
        ).astype(jnp.bfloat16)
        if by_columns:
            kept = lax.all_to_all(
                kept, "dp", 0, 0, axis_index_groups=tp_groups, tiled=True
            )
            kept = kept.transpose(1, 0, 2).reshape(half, TP * columns)
        else:
            kept = kept[0]
        other = lax.ppermute(kept, "seq", swap)
        return jnp.stack(
            [
                jnp.where(seq_index == 0, kept, other),
                jnp.where(seq_index == 0, other, kept),
            ]
        )

    def owned(early, late):
        other = lax.ppermute(jnp.where(first, late, early), "section", swap)
        return jnp.concatenate(
            [jnp.where(first, early, other), jnp.where(first, other, late)], axis=1
        ).astype(jnp.float32)[None]

    middle_rows, early_saved = forward(0, start_rows)
    final_rows, late_saved = forward(1, middle_rows)
    cot_rows = to_work(image_cot, text_cot).astype(jnp.float32)
    late_in, late_mod, late_gain, late_bias, late_weights = backward(1, cot_rows, late_saved)
    late_low = late_in.astype(jnp.bfloat16)
    late_settled = [settle(late_weights[k], k in (0, 2)) for k in range(4)]
    early_in, early_mod, early_gain, early_bias, early_weights = backward(
        0, late_low.astype(jnp.float32), early_saved
    )
    early_settled = [settle(early_weights[k], k in (0, 2)) for k in range(4)]
    weight_outs = [owned(early_settled[k], late_settled[k]) for k in range(4)]

    def to_owner(early, late):
        other = lax.ppermute(jnp.where(first, late, early), "section", swap)
        both = jnp.stack([jnp.where(first, early, other), jnp.where(first, other, late)])
        return lax.ppermute(both, ("dp", "seq"), trade)

    act_all = to_owner(middle_rows, final_rows)
    grad_all = to_owner(early_in.astype(jnp.bfloat16), late_low).astype(jnp.float32)
    image_out = act_all[:, :image_rows][None, :, None]
    text_out = act_all[:, image_rows:][None, :, None]
    image_grad = grad_all[:, :image_rows][None, :, None]
    text_grad = grad_all[:, image_rows:][None, :, None]

    def bias_total(parts_early, parts_late):
        early = jnp.concatenate(parts_early, axis=1)
        late = jnp.concatenate(parts_late, axis=1)
        own = jnp.where(first, early, late) + lax.ppermute(
            jnp.where(first, late, early), "section", swap
        )
        own = own + lax.ppermute(own, "seq", swap)
        if groups > 1:
            own = lax.psum(own, "dp", axis_index_groups=row_groups)
        outs = []
        start = 0
        for value in parts_early:
            size = value.shape[1]
            share = size // groups
            outs.append(
                lax.dynamic_slice_in_dim(
                    own[:, start : start + size], group_index * share, share, 1
                )[None]
            )
            start += size
        return outs

    bias_outs = bias_total(early_bias, late_bias)

    def mod_pack(mod_grad, gain_grad):
        row = jnp.zeros((1, width), jnp.float32).at[0, : 4 * HD].set(gain_grad.reshape(-1))
        return jnp.concatenate([mod_grad.reshape(12, width), row])

    early_pack = mod_pack(early_mod, early_gain)
    late_pack = mod_pack(late_mod, late_gain)
    own_mod = jnp.where(first, early_pack, late_pack).astype(jnp.bfloat16)
    other_mod = lax.ppermute(
        jnp.where(first, late_pack, early_pack).astype(jnp.bfloat16), "section", swap
    )
    mod_both = jnp.stack([jnp.where(first, own_mod, other_mod), jnp.where(first, other_mod, own_mod)])
    every_mod = lax.all_gather(mod_both, ("dp", "seq"), axis=0, tiled=True)
    every_mod = every_mod.reshape(data_parts, 2, batches, 13, width)
    place = jnp.arange(data_parts)
    place_tp = place // groups
    held_dp = (
        (place_tp - place_tp % 2)[:, None] + jnp.arange(2)[None, :]
    ) * groups + (place % groups)[:, None]
    every_ids = jnp.take(seq_table, held_dp.reshape(-1), axis=0).reshape(-1)
    every_cond = jax.nn.silu(jnp.take(cond_table, every_ids, axis=0).astype(jnp.float32)).astype(
        jnp.bfloat16
    )
    own_share = mod_weight.shape[2]
    every_cols = lax.dynamic_slice_in_dim(every_cond, dp_index * own_share, own_share, 1)
    mod_flat = every_mod[:, :, :, :12].reshape(-1, 2, 6 * width)
    modw_grad = jnp.einsum(
        "rd,rsk->sdk", every_cols, mod_flat, preferred_element_type=jnp.float32
    )[None]
    bias_share = mod_bias.shape[2]
    modb_grad = jnp.sum(
        lax.dynamic_slice_in_dim(mod_flat, dp_index * bias_share, bias_share, 2).astype(
            jnp.float32
        ),
        axis=0,
    )[None]
    gain_total = jnp.sum(every_mod[:, :, :, 12, : 4 * HD].astype(jnp.float32), axis=(0, 1, 2))
    gain_share = qk_gain.shape[2]
    gain_out = lax.dynamic_slice_in_dim(
        gain_total.reshape(2, 2 * HD), dp_index * gain_share, gain_share, 1
    )[None]
    return (
        image_out,
        text_out,
        image_grad,
        text_grad,
        modw_grad,
        modb_grad,
        weight_outs[0],
        bias_outs[0],
        gain_out,
        weight_outs[1],
        bias_outs[1],
        weight_outs[2],
        bias_outs[2],
        weight_outs[3],
        bias_outs[3],
    )


def solution(mesh):
    return jax.shard_map(
        body,
        mesh=mesh,
        in_specs=(
            P(None, "dp", "seq", None),
            P(None, "dp", "seq", None),
            P(None, "dp", "seq", None),
            P(None, "dp", "seq", None),
            P(),
            P(),
            P(None, "dp", None),
            P("section", None, "dp", None),
            P("section", None, "dp"),
            P("section", None, "dp", None),
            P("section", None, "dp"),
            P("section", None, "dp"),
            P("section", None, "dp", None),
            P("section", None, "dp"),
            P("section", None, "dp", None),
            P("section", None, "dp"),
            P("section", None, "dp", None),
            P("section", None, "dp"),
        ),
        out_specs=(
            P("section", None, "dp", "seq", None),
            P("section", None, "dp", "seq", None),
            P("section", None, "dp", "seq", None),
            P("section", None, "dp", "seq", None),
            P("section", None, "dp", None),
            P("section", None, "dp"),
            P("section", None, "dp", None),
            P("section", None, "dp"),
            P("section", None, "dp"),
            P("section", None, "dp", None),
            P("section", None, "dp"),
            P("section", None, "dp", None),
            P("section", None, "dp"),
            P("section", None, "dp", None),
            P("section", None, "dp"),
        ),
        check_vma=False,
    )
```
